32 devices in a mesh: rep: 2 (over x), exp: 2 (over core), tp: 8 (over z, y).
Axes of the slice: x: 2, y: 2, z: 4, core: 2. Of those that a mesh axis runs over, the one named last changes fastest.
Arguments:
- tokens: bfloat16 [1024, 4096], P(('rep', 'exp'), 'tp'), parts along dimension 0
- smooth_in: float32 [4096], P('tp'), may hold values from 0.5 to 2
- expert_ids: int32 [1024, 2], P(('rep', 'exp')), parts along dimension 0, may hold values from 0 to 3, as said below
- gate_fixed: int32 [1024, 2], P(('rep', 'exp')), parts along dimension 0, may hold values from 1 to 32767
- slots: int32 [1024, 2], P(('rep', 'exp')), parts along dimension 0, may hold values from 0 to 255, as said below
- w_gate: bfloat16 [4, 4096, 7168], P('exp', None, 'tp')
- w_up: bfloat16 [4, 4096, 7168], P('exp', None, 'tp')
- w_down: bfloat16 [4, 7168, 4096], P('exp', 'tp')
- gate_scale: float32 [4, 7168], P('exp', 'tp'), may hold values from 0.00010557433 to 0.0004222973
- up_scale: float32 [4, 7168], P('exp', 'tp'), may hold values from 0.00010557433 to 0.0004222973
- smooth_mid: float32 [4, 7168], P('exp', 'tp'), may hold values from 0.5 to 2
- down_scale: float32 [4, 4096], P('exp'), may hold values from 0.00015961338 to 0.0006384535
Outputs:
- moe_out: bfloat16 [1024, 4096], P(('rep', 'exp'), 'tp'), parts along dimension 0
The draws below stay inside these ranges and needn't reach their ends.
There are 2 independent parts, one for each index of `rep`. The reference program is written for one: setup_inputs(seed, part) draws one part's arguments, and reference() takes and returns one part's arrays. A program takes and returns all parts, laid end to end along the dimension named above; an argument that names none is the same for every part. Nothing has to cross between parts.
Inputs may be any that keep to these rules, and one draw needn't show every extreme that they name: `expert_ids`: the two experts of a token differ. Within one aligned block of 256 tokens (the tokens of one index of exp), the slots of the pairs that name one expert are distinct and run from 0 to their number less one. In every block some expert is named by 192 or more tokens.
All inputs are finite; a program needn't handle non-finite values.
Results may differ from the reference program's by a relative error of at most 0.006.
Values may be sent and summed in bfloat16 or wider, within the bound.
A program may use at most 128 MiB of HBM per device.

```python
import math
import jax
import jax.numpy as jnp
from jax import lax

D = 4096
FF = 7168
TOP = 2
BLK = 256
EXPERTS = 4
CAP = 192
TOKENS = 512


def routing(key):
    routing_key = jax.random.fold_in(key, 11)
    subkeys = jax.random.split(routing_key, 7)
    blocks = TOKENS // BLK
    hot_expert = jax.random.randint(subkeys[0], (), 0, EXPERTS)
    priority = jax.random.randint(subkeys[1], (blocks, BLK), 0, 1 << 20) * BLK + jnp.arange(BLK, dtype=jnp.int32)[None, :]
    position = jnp.argsort(jnp.argsort(priority, axis=1, stable=True), axis=1, stable=True)
    coin_flip = jax.random.randint(subkeys[2], (blocks, BLK), 0, 2)
    with_hot = ((position < CAP) | (coin_flip == 1)).reshape(TOKENS)
    first_off = jax.random.randint(subkeys[3], (TOKENS,), 1, EXPERTS)
    second_off = 1 + (first_off - 1 + jax.random.randint(subkeys[4], (TOKENS,), 1, EXPERTS - 1)) % (EXPERTS - 1)
    other_a = (hot_expert + first_off) % EXPERTS
    other_b = (hot_expert + second_off) % EXPERTS
    pair_one = jnp.where(with_hot, hot_expert, other_b)
    pair_two = other_a
    order_flip = jax.random.randint(subkeys[5], (TOKENS,), 0, 2)
    first = jnp.where(order_flip == 1, pair_two, pair_one)
    second = jnp.where(order_flip == 1, pair_one, pair_two)
    expert_list = jnp.stack([first, second], axis=1).astype(jnp.int32)
    slot_priority = jax.random.randint(subkeys[6], (blocks, 2 * BLK), 0, 1 << 20) * (2 * BLK) + jnp.arange(2 * BLK, dtype=jnp.int32)[None, :]
    flat_ids = expert_list.reshape(blocks, 2 * BLK)
    same_expert = flat_ids[:, :, None] == flat_ids[:, None, :]
    earlier = slot_priority[:, None, :] < slot_priority[:, :, None]
    slot_list = jnp.sum((same_expert & earlier).astype(jnp.int32), axis=2).reshape(TOKENS, 2)
    return (expert_list, slot_list.astype(jnp.int32))


def draw_expert_ids(key, part):
    expert_list, slot_list = routing(key)
    return expert_list


def draw_slots(key, part):
    expert_list, slot_list = routing(key)
    return slot_list


def int_weights(key, shape):
    return jax.random.randint(key, shape, -127, 128).astype(jnp.float32).astype(jnp.bfloat16)


def draw_w_gate(key, part):
    return int_weights(jax.random.fold_in(key, 1), (EXPERTS, D, FF))


def draw_w_up(key, part):
    return int_weights(jax.random.fold_in(key, 2), (EXPERTS, D, FF))


def draw_w_down(key, part):
    return int_weights(jax.random.fold_in(key, 3), (EXPERTS, FF, D))


def draw_tokens(key, part):
    subkeys = jax.random.split(jax.random.fold_in(key, 4), 3)
    column_scale = jnp.exp(jax.random.uniform(subkeys[0], (D,), jnp.float32, math.log(0.3), math.log(3.0)))
    row_scale = jnp.exp(jax.random.uniform(subkeys[1], (TOKENS, 1), jnp.float32, math.log(0.5), math.log(2.0)))
    values = jax.random.normal(subkeys[2], (TOKENS, D), jnp.float32)
    return (values * column_scale[None, :] * row_scale).astype(jnp.bfloat16)


def touch_ends(entries, own_key, smallest, high):
    longest = entries.shape.index(max(entries.shape))
    spots = []
    for shift in (0, 1):
        where = [jax.random.randint(jax.random.fold_in(own_key, axis), (), 0, length) for axis, length in enumerate(entries.shape)]
        where[longest] = (where[longest] + shift) % entries.shape[longest]
        spots.append(tuple(where))
    return entries.at[spots[0]].set(smallest).at[spots[1]].set(high)


def levels(rng, extent, cuts, least, top_value):
    def one(dim, blocks):
        draws = jax.random.uniform(jax.random.fold_in(jax.random.fold_in(rng, 6), dim), (blocks,), jnp.float32, least / len(cuts), top_value / len(cuts))
        return jnp.repeat(jnp.exp(draws), extent[dim] // blocks).reshape((-1,) + (1,) * (len(extent) - dim - 1))

    level = one(*cuts[0])
    for cut in cuts[1:]:
        level = level * one(*cut)
    return level


def setup_inputs(seed: int = 0, part: int = 0) -> dict:
    key_list = jax.random.split(jax.random.key(seed), 13)
    part_keys = jax.random.split(jax.random.fold_in(key_list[12], part), 13)
    return {
        "tokens": draw_tokens(jax.random.fold_in(jax.random.fold_in(key_list[12], part), 71), part),
        "smooth_in": jnp.clip(jnp.exp(math.log(2.0) - 1.3862944 * jax.random.uniform(key_list[1], (D,), jnp.float32) ** levels(key_list[1], (D,), ((0, 8),), -0.2, 0.2)), 0.5, 2.0),
        "expert_ids": draw_expert_ids(jax.random.fold_in(jax.random.fold_in(key_list[12], part), 71), part),
        "gate_fixed": touch_ends(jax.random.randint(part_keys[3], (TOKENS, TOP), 1, 32768), jax.random.fold_in(part_keys[3], 1), 1, 32767).astype(jnp.int32),
        "slots": draw_slots(jax.random.fold_in(jax.random.fold_in(key_list[12], part), 71), part),
        "w_gate": draw_w_gate(jax.random.fold_in(key_list[12], 71), part),
        "w_up": draw_w_up(jax.random.fold_in(key_list[12], 71), part),
        "w_down": draw_w_down(jax.random.fold_in(key_list[12], 71), part),
        "gate_scale": jnp.clip(jnp.exp(math.log(0.0004222973) - 1.3862944 * jax.random.uniform(key_list[8], (EXPERTS, FF), jnp.float32) ** levels(key_list[8], (EXPERTS, FF), ((0, 2), (1, 8)), -0.2, 0.2)), 0.00010557433, 0.0004222973),
        "up_scale": jnp.clip(jnp.exp(math.log(0.0004222973) - 1.3862944 * jax.random.uniform(key_list[9], (EXPERTS, FF), jnp.float32) ** levels(key_list[9], (EXPERTS, FF), ((0, 2), (1, 8)), -0.2, 0.2)), 0.00010557433, 0.0004222973),
        "smooth_mid": jnp.clip(jnp.exp(math.log(2.0) - 1.3862944 * jax.random.uniform(key_list[10], (EXPERTS, FF), jnp.float32) ** levels(key_list[10], (EXPERTS, FF), ((0, 2), (1, 8)), -0.2, 0.2)), 0.5, 2.0),
        "down_scale": jnp.clip(jnp.exp(math.log(0.0006384535) - 1.3862944 * jax.random.uniform(key_list[11], (EXPERTS, D), jnp.float32) ** levels(key_list[11], (EXPERTS, D), ((0, 2),), -0.2, 0.2)), 0.00015961338, 0.0006384535),
    }


CLIP_RATIO = 0.35
EPSILON = 1e-6


def expert_rows(quantized, in_scale, weights_of):
    gate_e, up_e, down_e, gate_sc, up_sc, smooth_e, down_sc = weights_of
    gate_pre = jnp.dot(quantized, gate_e, preferred_element_type=jnp.float32) * in_scale[:, None] * gate_sc[None, :]
    up_pre = jnp.dot(quantized, up_e, preferred_element_type=jnp.float32) * in_scale[:, None] * up_sc[None, :]
    hidden = jax.nn.silu(gate_pre) * up_pre / smooth_e[None, :]
    mid_scale = CLIP_RATIO * (jnp.max(jnp.abs(hidden), axis=1) + EPSILON) / 127.0
    hidden_q = jnp.clip(hidden / mid_scale[:, None], -127.0, 127.0).astype(jnp.bfloat16)
    down_acc = jnp.dot(hidden_q, down_e, preferred_element_type=jnp.float32)
    return down_acc * mid_scale[:, None] * down_sc[None, :]


def reference(tokens, smooth_in, expert_ids, gate_fixed, slots, w_gate, w_up, w_down, gate_scale, up_scale, smooth_mid, down_scale):
    smoothed = tokens.astype(jnp.float32) / smooth_in[None, :]
    in_scale = CLIP_RATIO * (jnp.max(jnp.abs(smoothed), axis=1) + EPSILON) / 127.0
    quantized = jnp.clip(smoothed / in_scale[:, None], -127.0, 127.0).astype(jnp.bfloat16)
    gate_values = gate_fixed.astype(jnp.float32)
    weight = gate_values / jnp.sum(gate_values, axis=1, keepdims=True)
    pair_weight = jnp.where(slots < CAP, weight, jnp.zeros_like(weight))

    def add_expert(accumulated, expert_index):
        weights_of = (w_gate[expert_index], w_up[expert_index], w_down[expert_index],
                      gate_scale[expert_index], up_scale[expert_index], smooth_mid[expert_index], down_scale[expert_index])
        produced = expert_rows(quantized, in_scale, weights_of)
        share = jnp.sum(jnp.where(expert_ids == expert_index, pair_weight, jnp.zeros_like(pair_weight)), axis=1)
        return accumulated + produced * share[:, None], expert_index

    start_sum = jnp.zeros((TOKENS, D), jnp.float32)
    accumulated, unused = lax.scan(add_expert, start_sum, jnp.arange(EXPERTS, dtype=jnp.int32))
    return accumulated.astype(jnp.bfloat16)
```

```python
import functools

import jax
import jax.numpy as jnp
from jax import lax
from jax.experimental import pallas as pl
from jax.experimental.pallas import tpu as pltpu
from jax.sharding import PartitionSpec as P

CLIP_RATIO = 0.35
EPSILON = 1e-06
LANES = 128
SPLIT = (1, 1)
MESH = pl.DeviceIdType.MESH
F32 = jnp.float32
BF16 = jnp.bfloat16


def kernel(
    n, capacity, sizes,
    tok_ref, smooth_ref, ids_ref, gate_ref, slot_ref, wg_ref, wu_ref, wd_ref, gs_ref, us_ref, sm_ref, ds_ref,
    out_ref,
    x, xq, wbuf, dbuf, acc, h, hq, meta_rows, meta, coef, pk, hx, hm, own, ssend, srecv, comb, yrecv, zrecv,
    w_sem, d_sem, pk_s, pk_r, hx_s, hx_r, meta_s, meta_r,
    ao_s, az_s, ay_s, as_s, ag_r, as_r, rs_s, rs_r, ry_s, ry_r, rz_s, rz_r,
):
    q = n // 2
    me = lax.axis_index("tp")
    core = lax.axis_index("exp")
    z, y = me // 2, me % 2
    direction = 1 - 2 * (z % 2)
    experts, _, width = wg_ref.shape
    block, depth = tok_ref.shape
    groups = len(sizes)
    offsets = [sum(sizes[:g]) for g in range(groups)]
    halves = wbuf.shape[0]
    tiles = [(c, min(LANES, width - c)) for c in range(0, width, LANES)]

    def rows_of(g):
        return pl.ds(offsets[g], sizes[g])

    def z_of(j):
        return (z + direction * j + q) % q

    def chunk(j, other):
        return z_of(j) * 2 + y + other * (1 - 2 * y)

    upper = (2 * z) // q
    near_count = z * (1 - upper) + (q - 1 - z) * upper

    def side(t):
        near = (2 * near_count - t + 4 * q) // (4 * q)
        return near * (1 - 2 * (t % 2)) + (1 - near) * (1 - 2 * upper)

    def line(t):
        near = (2 * near_count - t + 4 * q) // (4 * q)
        return z + side(t) * (near * ((t + 1) // 2) + (1 - near) * (t - near_count))

    def slab(t, other):
        return line(t) * 2 + y + other * (1 - 2 * y)

    def remote(src, dst, send, recv, device):
        return pltpu.make_async_remote_copy(
            src_ref=src, dst_ref=dst, send_sem=send, recv_sem=recv,
            device_id=device, device_id_type=MESH,
        )

    sibling = {"exp": 1 - core}
    partner = {"tp": chunk(0, 1)}

    def chunk_rows(p):
        return pl.ds(pl.multiple_of(p * depth, depth), depth)

    def weight_copies(k):
        rows = chunk_rows(slab(k // 2, k % 2))
        if halves == 1:
            dsts = [wbuf.at[0, :, rows, pl.ds(i * width, width)] for i in range(2)]
        else:
            dsts = [wbuf.at[i, :, rows, :] for i in range(2)]
        return [
            pltpu.make_async_copy(ref.at[:, rows, :], dst, w_sem.at[k, i])
            for i, (ref, dst) in enumerate(zip((wg_ref, wu_ref), dsts))
        ]

    def down_copy(e):
        return pltpu.make_async_copy(wd_ref.at[e], dbuf.at[e], d_sem.at[e])

    barrier = pltpu.get_barrier_semaphore()
    pl.semaphore_signal(barrier, inc=1, device_id=sibling, device_id_type=MESH)

    @pl.loop(1, n)
    def _(d):
        pl.semaphore_signal(barrier, inc=1, device_id={"tp": (me + d) % n}, device_id_type=MESH)

    @pl.loop(0, n)
    def _(k):
        for copy in weight_copies(k):
            copy.start()

    for e in range(experts):
        down_copy(e).start()

    x[me, 0] = tok_ref[...]
    smooth = smooth_ref[...]
    peak = jnp.max(jnp.abs(tok_ref[...].astype(F32) / smooth), axis=1, keepdims=True)
    peak_row = jnp.broadcast_to(peak, (block, LANES)).T[0:1, :]
    pk[pl.ds(me, 1), :, 0:block] = peak_row[None]
    pk[pl.ds(me, 1), :, block:] = smooth[None]

    pl.semaphore_wait(barrier, n)

    def pk_copy(d):
        return remote(pk.at[me], pk.at[me], pk_s.at[d], pk_r.at[me], {"tp": (me + d) % n})

    def piece(g, p, b):
        return x.at[p, b, rows_of(g), :]

    def own_copy(g, up):
        part = piece(g, me, 0)
        return remote(part, part, ao_s.at[g, up], ag_r.at[g, me], {"tp": me + 4 * up - 2})

    def relay_copy(g, p, step):
        part = piece(g, p, 0)
        return remote(part, part, az_s.at[g, p // 2], ag_r.at[g, p], {"tp": me - 2 * step})

    def y_copy(g, p):
        part = piece(g, p, 0)
        return remote(part, part, ay_s.at[g, p // 2], ag_r.at[g, p], partner)

    def sib_copy(g, p):
        return remote(piece(g, p, 0), piece(g, p, 1), as_s.at[g, p], as_r.at[g, p], sibling)

    def arrived(g, p):
        remote(piece(g, p, 0), piece(g, p, 0), as_s.at[g, p], ag_r.at[g, p], sibling).wait_recv()

    def guard_own(act):
        for up, there in enumerate((z > 0, z < q - 1)):

            @pl.when(there)
            def _():
                act(up)

    def guard_slabs(s, act):
        for step in (-1, 1):
            source = z + step * s

            @pl.when((source >= 0) & (source < q))
            def _():
                act(me + 2 * step * s, step)

    def guard_relay(g, p, step, act):
        target = z - step

        @pl.when((target >= 0) & (target < q))
        def _():
            act(relay_copy(g, p, step))

    def begin(g):
        y_copy(g, me).start()
        guard_own(lambda up: own_copy(g, up).start())
        sib_copy(g, me).start()

    def across(g, s):
        def act(p, step):
            arrived(g, p)
            guard_relay(g, p, step, lambda copy: copy.start())
            y_copy(g, p).start()
            sib_copy(g, p).start()

        guard_slabs(s, act)

    def beside(g, t):
        p = slab(t, 1)
        arrived(g, p)
        sib_copy(g, p).start()

    begin(0)

    @pl.loop(1, n)
    def _(d):
        pk_copy(d).start()

    if groups > 1:
        begin(1)

    gates = gate_ref[...].astype(F32)
    total = jnp.sum(gates, axis=0, keepdims=True)
    weight = jnp.where(slot_ref[...] < capacity, gates / total, 0.0)

    def share_of(expert):
        return jnp.sum(jnp.where(ids_ref[...] == expert, weight, 0.0), axis=0, keepdims=True)

    @pl.loop(1, n)
    def _(d):
        p = (me + d) % n
        remote(pk.at[p], pk.at[p], pk_s.at[d], pk_r.at[p], {"tp": p}).wait_recv()

    row_peak = jnp.max(pk[0:n, :, 0:block], axis=0)
    in_scale = CLIP_RATIO * (row_peak + EPSILON) / 127.0
    inverse = 1.0 / in_scale
    for i, owner in enumerate((core, 1 - core)):
        for e in range(experts):
            meta_rows[i, e:e + 1, :] = share_of(owner * experts + e)
        meta_rows[i, experts:experts + 1, :] = in_scale
        meta_rows[i, experts + 1:experts + 2, :] = inverse
    meta_copy = remote(meta_rows.at[1], meta_rows.at[2], meta_s, meta_r, sibling)
    meta_copy.start()
    line_index = lax.broadcasted_iota(jnp.int32, (LANES, block), 0)

    def columns(slot):
        result = jnp.zeros((LANES, block), F32)
        for i in range(experts + 2):
            result = jnp.where(line_index == i, meta_rows[slot, i:i + 1, :], result)
        return result.T

    meta[0] = columns(0)
    meta_copy.wait_recv()
    meta[1] = columns(2)

    def compute(g, k, first):
        p = slab(k // 2, k % 2)
        rg = sizes[g]
        if g == 0:
            for copy in weight_copies(k):
                copy.wait()
        sib_copy(g, p).wait_recv()
        factor = 1.0 / pk[p][:, block:]
        for b in range(2):
            scale = meta[b, rows_of(g), experts + 1:experts + 2]
            scaled = x[p, b, rows_of(g), :].astype(F32) * factor * scale
            xq[b * rg:(b + 1) * rg, :] = jnp.clip(scaled, -127.0, 127.0).astype(BF16)
        for e in range(experts):
            for half in range(halves):
                product = jnp.dot(
                    xq[0:2 * rg, :], wbuf[half, e, chunk_rows(p), :], preferred_element_type=F32
                )
                if first:
                    acc[half, e, 0:2 * rg] = product
                else:
                    acc[half, e, 0:2 * rg] += product

    rb = 32

    def row_blocks(g, body):
        blocks = sizes[g] // rb

        @pl.loop(0, 2 * blocks)
        def _(r):
            rows = pl.ds(pl.multiple_of(r * rb, rb), rb)
            inner = pl.ds(pl.multiple_of(offsets[g] + (r % blocks) * rb, rb), rb)
            body(rows, meta[r // blocks, inner, :])

    def spread(column):
        return jnp.broadcast_to(column, (rb, LANES))

    def hidden(g):
        for e in range(experts):

            def body(rows, info):
                scale = spread(info[:, experts:experts + 1])
                largest = None
                for c, w in tiles:
                    cols = pl.ds(c, w)
                    gate_acc = acc[0, e, rows, cols]
                    up_acc = acc[0, e, rows, pl.ds(width + c, w)] if halves == 1 else acc[1, e, rows, cols]
                    gate = gate_acc * scale[:, 0:w] * gs_ref[:, cols][e:e + 1]
                    factor = us_ref[:, cols][e:e + 1] / sm_ref[:, cols][e:e + 1]
                    up = up_acc * scale[:, 0:w] * factor
                    value = gate / (1.0 + jnp.exp(-gate)) * up
                    h[e, rows, cols] = value
                    size = jnp.abs(value)
                    if w < LANES:
                        size = spread(jnp.max(size, axis=1, keepdims=True))
                    largest = size if largest is None else jnp.maximum(largest, size)
                hm[rows, :] = largest

            row_blocks(g, body)
            hx[g, pl.ds(me, 1), e:e + 1, 0:2 * sizes[g]] = jnp.max(
                hm[0:2 * sizes[g], :].T, axis=0, keepdims=True
            )[None]

        @pl.loop(1, n)
        def _(d):
            hx_copy(g, d).start()

    def hx_copy(g, d):
        return remote(
            hx.at[g, me], hx.at[g, me], hx_s.at[g, d], hx_r.at[g, me], {"tp": (me + d) % n}
        )

    def requantize(g):
        @pl.loop(1, n)
        def _(d):
            p = (me + d) % n
            remote(hx.at[g, p], hx.at[g, p], hx_s.at[g, d], hx_r.at[g, p], {"tp": p}).wait_recv()

        mid_rows = CLIP_RATIO * (jnp.max(hx[g, 0:n], axis=0) + EPSILON) / 127.0
        for e in range(experts):
            rows_m = 2 * sizes[g]
            coef[e, 0:rows_m, :] = jnp.broadcast_to(mid_rows[e:e + 1, 0:rows_m], (LANES, rows_m)).T

            def body(rows, info):
                mid = coef[e, rows, :]
                inv = 1.0 / mid
                for c, w in tiles:
                    scaled = h[e, rows, pl.ds(c, w)] * inv[:, 0:w]
                    hq[e, rows, pl.ds(c, w)] = jnp.clip(scaled, -127.0, 127.0).astype(BF16)
                coef[e, rows, :] = mid * spread(info[:, e:e + 1])

            row_blocks(g, body)

    def shard_of(k):
        return chunk(q - 1 - k % q, 1 - k // q)

    def rs_copy(g, k):
        return remote(
            ssend.at[k, rows_of(g), :], srecv.at[k, rows_of(g), :], rs_s.at[g, k], rs_r.at[g, k], sibling
        )

    def ry_copy(g, j):
        return remote(
            srecv.at[q - 1 - j, rows_of(g), :], yrecv.at[j, rows_of(g), :],
            ry_s.at[g, j], ry_r.at[g, j], partner,
        )

    def rz_copy(g, j):
        return remote(
            yrecv.at[j, rows_of(g), :], zrecv.at[z, rows_of(g), :],
            rz_s.at[g, j], rz_r.at[g, z], {"tp": chunk(j, 0)},
        )

    def combine(g, k):
        j = q - 1 - k % q
        rs_copy(g, k).wait_recv()
        mine = own[k % 2, 0:sizes[g], :]

        @pl.when(k < q)
        def _():
            srecv[k, rows_of(g), :] = (mine + srecv[k, rows_of(g), :].astype(F32)).astype(BF16)
            ry_copy(g, j).start()

        @pl.when(k >= q)
        def _():
            comb[j, rows_of(g), :] = mine + srecv[k, rows_of(g), :].astype(F32)

    def down(g, k):
        cols = chunk_rows(shard_of(k))
        rg = sizes[g]
        result = None
        for e in range(experts):
            part = jnp.dot(hq[e, 0:2 * rg, :], dbuf[e, :, cols], preferred_element_type=F32)
            part = part * coef[e, 0:2 * rg, 0:1] * ds_ref[:, cols][e:e + 1]
            result = part if result is None else result + part
        ssend[k, rows_of(g), :] = result[rg:].astype(BF16)
        rs_copy(g, k).start()
        own[k % 2, 0:rg, :] = result[0:rg]

        @pl.when(k > 0)
        def _():
            combine(g, k - 1)

    def finish(g, j):
        ry_copy(g, j).wait_recv()
        rows = rows_of(g)

        @pl.when(j > 0)
        def _():
            yrecv[j, rows, :] = (comb[j, rows, :] + yrecv[j, rows, :].astype(F32)).astype(BF16)
            rz_copy(g, j).start()

        @pl.when(j == 0)
        def _():
            comb[0, rows, :] += yrecv[0, rows, :].astype(F32)

    def final(g):
        rows = rows_of(g)

        @pl.loop(1, q)
        def _(j):
            s = z_of(j)
            part = zrecv.at[s, rows, :]
            remote(part, part, rz_s.at[g, j], rz_r.at[g, s], sibling).wait_recv()
            comb[0, rows, :] += zrecv[s, rows, :].astype(F32)

        out_ref[rows, :] = comb[0, rows, :].astype(BF16)

    per_step = -(-n // (q - 1))
    last = groups - 1
    for g in range(groups):

        @pl.loop(0, q)
        def _(t):
            @pl.when(t > 0)
            def _():
                if g < last:
                    across(g + 1, t)

            @pl.when(t == 0)
            def _():
                compute(g, 0, True)

            @pl.when(t > 0)
            def _():
                compute(g, 2 * t, False)

            if g + 2 <= last:

                @pl.when(t == 1)
                def _():
                    begin(g + 2)

            if g == 0:

                @pl.when(t + 1 < q)
                def _():
                    across(0, t + 1)

                beside(0, t)
            else:

                @pl.when(t == q - 1)
                def _():
                    beside(g, t)

            if g < last:

                @pl.when(t > 0)
                def _():
                    beside(g + 1, t - 1)

            compute(g, 2 * t + 1, False)

            if g > 0:

                @pl.when(t == 1)
                def _():
                    requantize(g - 1)

                @pl.when(t >= 1)
                def _():
                    @pl.loop(0, per_step)
                    def _(i):
                        k = (t - 1) * per_step + i

                        @pl.when(k < n)
                        def _():
                            down(g - 1, k)

            if g > 1:
                finish(g - 2, q - 1 - t)

        if g == 0:
            for e in range(experts):
                down_copy(e).wait()
        hidden(g)
        if g > 0:
            combine(g - 1, n - 1)

    requantize(last)

    @pl.loop(0, n)
    def _(k):
        down(last, k)
        if last > 0:

            @pl.when(k >= q)
            def _():
                finish(last - 1, n - 1 - k)

    combine(last, n - 1)

    @pl.loop(0, q)
    def _(i):
        finish(last, q - 1 - i)

    for g in range(groups):
        final(g)

    meta_copy.wait_send()

    @pl.loop(1, n)
    def _(d):
        pk_copy(d).wait_send()

    for g in range(groups):
        guard_own(lambda up: own_copy(g, up).wait_send())

        @pl.loop(1, n)
        def _(d):
            hx_copy(g, d).wait_send()

        @pl.loop(0, n)
        def _(k):
            sib_copy(g, k).wait_send()
            rs_copy(g, k).wait_send()

        @pl.loop(0, q)
        def _(j):
            y_copy(g, slab(j, 0)).wait_send()
            ry_copy(g, j).wait_send()

        @pl.loop(1, q)
        def _(j):
            guard_slabs(
                j, lambda p, step: guard_relay(g, p, step, lambda copy: copy.wait_send())
            )
            rz_copy(g, j).wait_send()


def per_device(
    n,
    tokens, smooth_in, expert_ids, gate_fixed, slots,
    w_gate, w_up, w_down, gate_scale, up_scale, smooth_mid, down_scale,
):
    q = n // 2
    experts, features, width = w_gate.shape
    block, depth = tokens.shape
    sizes = tuple(block * part // sum(SPLIT) for part in SPLIT)
    groups = len(sizes)
    rows_m = 2 * max(sizes)
    packed = width % LANES == 0
    halves = 1 if packed else 2
    cols = 2 * width if packed else width
    vmem = pl.BlockSpec(memory_space=pltpu.VMEM)
    hbm = pl.BlockSpec(memory_space=pl.ANY)
    dma = pltpu.SemaphoreType.DMA
    slab = (block, depth)
    return pl.pallas_call(
        functools.partial(kernel, n, 3 * block // 4, sizes),
        out_shape=jax.ShapeDtypeStruct((block, depth), BF16),
        in_specs=[vmem] * 5 + [hbm] * 3 + [vmem] * 4,
        out_specs=vmem,
        scratch_shapes=[
            pltpu.VMEM((n, 2, *slab), BF16),
            pltpu.VMEM((rows_m, depth), BF16),
            pltpu.VMEM((halves, experts, features, cols), BF16),
            pltpu.VMEM((experts, width, features), BF16),
            pltpu.VMEM((halves, experts, rows_m, cols), F32),
            pltpu.VMEM((experts, rows_m, width), F32),
            pltpu.VMEM((experts, rows_m, width), BF16),
            pltpu.VMEM((4, 8, block), F32),
            pltpu.VMEM((2, block, LANES), F32),
            pltpu.VMEM((experts, rows_m, LANES), F32),
            pltpu.VMEM((n + 8, 1, block + depth), F32),
            pltpu.VMEM((groups, n + 8, experts, rows_m), F32),
            pltpu.VMEM((rows_m, LANES), F32),
            pltpu.VMEM((2, max(sizes), depth), F32),
            pltpu.VMEM((n, *slab), BF16),
            pltpu.VMEM((n, *slab), BF16),
            pltpu.VMEM((q, *slab), F32),
            pltpu.VMEM((q, *slab), BF16),
            pltpu.VMEM((q, *slab), BF16),
            dma((n, 2)), dma((experts,)), dma((n,)), dma((n,)), dma((groups, n)), dma((groups, n)), dma, dma,
            dma((groups, 2)), dma((groups, q)), dma((groups, q)), dma((groups, n)), dma((groups, n)), dma((groups, n)),
            dma((groups, n)), dma((groups, n)), dma((groups, q)), dma((groups, q)), dma((groups, q)), dma((groups, q)),
        ],
        compiler_params=pltpu.CompilerParams(
            collective_id=0, has_side_effects=True, vmem_limit_bytes=67043328
        ),
    )(
        tokens, smooth_in[None, :], expert_ids.T, gate_fixed.T, slots.T,
        w_gate, w_up, w_down, gate_scale, up_scale, smooth_mid, down_scale,
    )


def solution(mesh):
    n = mesh.shape["tp"]
    in_specs = (
        P(("rep", "exp"), "tp"),
        P("tp"),
        P(("rep", "exp"), None),
        P(("rep", "exp"), None),
        P(("rep", "exp"), None),
        P("exp", None, "tp"),
        P("exp", None, "tp"),
        P("exp", "tp", None),
        P("exp", "tp"),
        P("exp", "tp"),
        P("exp", "tp"),
        P("exp", None),
    )
    out_specs = P(("rep", "exp"), "tp")
    return jax.shard_map(
        functools.partial(per_device, n), mesh=mesh, in_specs=in_specs, out_specs=out_specs, check_vma=False
    )
```

```python
import functools

import jax
import jax.numpy as jnp
from jax import lax
from jax.experimental import pallas as pl
from jax.experimental.pallas import tpu as pltpu
from jax.sharding import PartitionSpec as P

CLIP_RATIO = 0.35
EPSILON = 1e-06
LANES = 128
SPLIT = (1, 1)
MESH = pl.DeviceIdType.MESH
F32 = jnp.float32
BF16 = jnp.bfloat16


def kernel(
    n, capacity, sizes,
    tok_ref, smooth_ref, ids_ref, gate_ref, slot_ref, wg_ref, wu_ref, wd_ref, gs_ref, us_ref, sm_ref, ds_ref,
    out_ref,
    x, xq, wbuf, dbuf, acc, h, hq, meta_rows, meta, coef, pk, hx, hm, own, ssend, srecv, comb, yrecv, zrecv,
    w_sem, d_sem, pk_s, pk_r, hx_s, hx_r, meta_s, meta_r,
    ao_s, az_s, ay_s, as_s, ag_r, as_r, rs_s, rs_r, ry_s, ry_r, rz_s, rz_r,
):
    q = n // 2
    me = lax.axis_index("tp")
    core = lax.axis_index("exp")
    z, y = me // 2, me % 2
    direction = 1 - 2 * (z % 2)
    experts, _, width = wg_ref.shape
    block, depth = tok_ref.shape
    groups = len(sizes)
    offsets = [sum(sizes[:g]) for g in range(groups)]
    halves = wbuf.shape[0]
    tiles = [(c, min(LANES, width - c)) for c in range(0, width, LANES)]

    def rows_of(g):
        return pl.ds(offsets[g], sizes[g])

    def z_of(j):
        return (z + direction * j + q) % q

    def chunk(j, other):
        return z_of(j) * 2 + y + other * (1 - 2 * y)

    upper = (2 * z) // q
    near_count = z * (1 - upper) + (q - 1 - z) * upper

    def side(t):
        near = (2 * near_count - t + 4 * q) // (4 * q)
        return near * (1 - 2 * (t % 2)) + (1 - near) * (1 - 2 * upper)

    def line(t):
        near = (2 * near_count - t + 4 * q) // (4 * q)
        return z + side(t) * (near * ((t + 1) // 2) + (1 - near) * (t - near_count))

    def slab(t, other):
        return line(t) * 2 + y + other * (1 - 2 * y)

    def remote(src, dst, send, recv, device):
        return pltpu.make_async_remote_copy(
            src_ref=src, dst_ref=dst, send_sem=send, recv_sem=recv,
            device_id=device, device_id_type=MESH,
        )

    sibling = {"exp": 1 - core}
    partner = {"tp": chunk(0, 1)}

    def chunk_rows(p):
        return pl.ds(pl.multiple_of(p * depth, depth), depth)

    def weight_copies(k):
        rows = chunk_rows(slab(k // 2, k % 2))
        if halves == 1:
            dsts = [wbuf.at[0, :, rows, pl.ds(i * width, width)] for i in range(2)]
        else:
            dsts = [wbuf.at[i, :, rows, :] for i in range(2)]
        return [
            pltpu.make_async_copy(ref.at[:, rows, :], dst, w_sem.at[k, i])
            for i, (ref, dst) in enumerate(zip((wg_ref, wu_ref), dsts))
        ]

    def down_copy(e):
        return pltpu.make_async_copy(wd_ref.at[e], dbuf.at[e], d_sem.at[e])

    barrier = pltpu.get_barrier_semaphore()
    pl.semaphore_signal(barrier, inc=1, device_id=sibling, device_id_type=MESH)

    @pl.loop(1, n)
    def _(d):
        pl.semaphore_signal(barrier, inc=1, device_id={"tp": (me + d) % n}, device_id_type=MESH)

    @pl.loop(0, n)
    def _(k):
        for copy in weight_copies(k):
            copy.start()

    for e in range(experts):
        down_copy(e).start()

    x[me, 0] = tok_ref[...]
    smooth = smooth_ref[...]
    peak = jnp.max(jnp.abs(tok_ref[...].astype(F32) / smooth), axis=1, keepdims=True)
    peak_row = jnp.broadcast_to(peak, (block, LANES)).T[0:1, :]
    pk[pl.ds(me, 1), :, 0:block] = peak_row[None]
    pk[pl.ds(me, 1), :, block:] = smooth[None]

    pl.semaphore_wait(barrier, n)

    def pk_copy(d):
        return remote(pk.at[me], pk.at[me], pk_s.at[d], pk_r.at[me], {"tp": (me + d) % n})

    def piece(g, p, b):
        return x.at[p, b, rows_of(g), :]

    def own_copy(g, up):
        part = piece(g, me, 0)
        return remote(part, part, ao_s.at[g, up], ag_r.at[g, me], {"tp": me + 4 * up - 2})

    def relay_copy(g, p, step):
        part = piece(g, p, 0)
        return remote(part, part, az_s.at[g, p // 2], ag_r.at[g, p], {"tp": me - 2 * step})

    def y_copy(g, p):
        part = piece(g, p, 0)
        return remote(part, part, ay_s.at[g, p // 2], ag_r.at[g, p], partner)

    def sib_copy(g, p):
        return remote(piece(g, p, 0), piece(g, p, 1), as_s.at[g, p], as_r.at[g, p], sibling)

    def arrived(g, p):
        remote(piece(g, p, 0), piece(g, p, 0), as_s.at[g, p], ag_r.at[g, p], sibling).wait_recv()

    def guard_own(act):
        for up, there in enumerate((z > 0, z < q - 1)):

            @pl.when(there)
            def _():
                act(up)

    def guard_slabs(s, act):
        for step in (-1, 1):
            source = z + step * s

            @pl.when((source >= 0) & (source < q))
            def _():
                act(me + 2 * step * s, step)

    def guard_relay(g, p, step, act):
        target = z - step

        @pl.when((target >= 0) & (target < q))
        def _():
            act(relay_copy(g, p, step))

    def begin(g):
        y_copy(g, me).start()
        guard_own(lambda up: own_copy(g, up).start())
        sib_copy(g, me).start()

    def across(g, s):
        def act(p, step):
            arrived(g, p)
            guard_relay(g, p, step, lambda copy: copy.start())
            y_copy(g, p).start()
            sib_copy(g, p).start()

        guard_slabs(s, act)

    def beside(g, t):
        p = slab(t, 1)
        arrived(g, p)
        sib_copy(g, p).start()

    begin(0)

    @pl.loop(1, n)
    def _(d):
        pk_copy(d).start()

    if groups > 1:
        begin(1)

    gates = gate_ref[...].astype(F32)
    total = jnp.sum(gates, axis=0, keepdims=True)
    weight = jnp.where(slot_ref[...] < capacity, gates / total, 0.0)

    def share_of(expert):
        return jnp.sum(jnp.where(ids_ref[...] == expert, weight, 0.0), axis=0, keepdims=True)

    @pl.loop(1, n)
    def _(d):
        p = (me + d) % n
        remote(pk.at[p], pk.at[p], pk_s.at[d], pk_r.at[p], {"tp": p}).wait_recv()

    row_peak = jnp.max(pk[0:n, :, 0:block], axis=0)
    in_scale = CLIP_RATIO * (row_peak + EPSILON) / 127.0
    inverse = 1.0 / in_scale
    for i, owner in enumerate((core, 1 - core)):
        for e in range(experts):
            meta_rows[i, e:e + 1, :] = share_of(owner * experts + e)
        meta_rows[i, experts:experts + 1, :] = in_scale
        meta_rows[i, experts + 1:experts + 2, :] = inverse
    meta_copy = remote(meta_rows.at[1], meta_rows.at[2], meta_s, meta_r, sibling)
    meta_copy.start()
    line_index = lax.broadcasted_iota(jnp.int32, (LANES, block), 0)

    def columns(slot):
        result = jnp.zeros((LANES, block), F32)
        for i in range(experts + 2):
            result = jnp.where(line_index == i, meta_rows[slot, i:i + 1, :], result)
        return result.T

    meta[0] = columns(0)
    meta_copy.wait_recv()
    meta[1] = columns(2)

    def compute(g, k, first):
        p = slab(k // 2, k % 2)
        rg = sizes[g]
        if g == 0:
            for copy in weight_copies(k):
                copy.wait()
        sib_copy(g, p).wait_recv()
        factor = 1.0 / pk[p][:, block:]
        for b in range(2):
            scale = meta[b, rows_of(g), experts + 1:experts + 2]
            scaled = x[p, b, rows_of(g), :].astype(F32) * factor * scale
            xq[b * rg:(b + 1) * rg, :] = jnp.clip(scaled, -127.0, 127.0).astype(BF16)
        for e in range(experts):
            for half in range(halves):
                product = jnp.dot(
                    xq[0:2 * rg, :], wbuf[half, e, chunk_rows(p), :], preferred_element_type=F32
                )
                if first:
                    acc[half, e, 0:2 * rg] = product
                else:
                    acc[half, e, 0:2 * rg] += product

    rb = 32

    def row_blocks(g, body):
        blocks = sizes[g] // rb

        @pl.loop(0, 2 * blocks)
        def _(r):
            rows = pl.ds(pl.multiple_of(r * rb, rb), rb)
            inner = pl.ds(pl.multiple_of(offsets[g] + (r % blocks) * rb, rb), rb)
            body(rows, meta[r // blocks, inner, :])

    def spread(column):
        return jnp.broadcast_to(column, (rb, LANES))

    def hidden(g):
        for e in range(experts):

            def body(rows, info):
                scale = spread(info[:, experts:experts + 1])
                largest = None
                for c, w in tiles:
                    cols = pl.ds(c, w)
                    gate_acc = acc[0, e, rows, cols]
                    up_acc = acc[0, e, rows, pl.ds(width + c, w)] if halves == 1 else acc[1, e, rows, cols]
                    gate = gate_acc * scale[:, 0:w] * gs_ref[:, cols][e:e + 1]
                    factor = us_ref[:, cols][e:e + 1] / sm_ref[:, cols][e:e + 1]
                    up = up_acc * scale[:, 0:w] * factor
                    value = gate / (1.0 + jnp.exp(-gate)) * up
                    h[e, rows, cols] = value
                    size = jnp.abs(value)
                    if w < LANES:
                        size = spread(jnp.max(size, axis=1, keepdims=True))
                    largest = size if largest is None else jnp.maximum(largest, size)
                hm[rows, :] = largest

            row_blocks(g, body)
            hx[g, pl.ds(me, 1), e:e + 1, 0:2 * sizes[g]] = jnp.max(
                hm[0:2 * sizes[g], :].T, axis=0, keepdims=True
            )[None]

        @pl.loop(1, n)
        def _(d):
            hx_copy(g, d).start()

    def hx_copy(g, d):
        return remote(
            hx.at[g, me], hx.at[g, me], hx_s.at[g, d], hx_r.at[g, me], {"tp": (me + d) % n}
        )

    def requantize(g):
        @pl.loop(1, n)
        def _(d):
            p = (me + d) % n
            remote(hx.at[g, p], hx.at[g, p], hx_s.at[g, d], hx_r.at[g, p], {"tp": p}).wait_recv()

        mid_rows = CLIP_RATIO * (jnp.max(hx[g, 0:n], axis=0) + EPSILON) / 127.0
        for e in range(experts):
            rows_m = 2 * sizes[g]
            coef[e, 0:rows_m, :] = jnp.broadcast_to(mid_rows[e:e + 1, 0:rows_m], (LANES, rows_m)).T

            def body(rows, info):
                mid = coef[e, rows, :]
                inv = 1.0 / mid
                for c, w in tiles:
                    scaled = h[e, rows, pl.ds(c, w)] * inv[:, 0:w]
                    hq[e, rows, pl.ds(c, w)] = jnp.clip(scaled, -127.0, 127.0).astype(BF16)
                coef[e, rows, :] = mid * spread(info[:, e:e + 1])

            row_blocks(g, body)

    def shard_of(k):
        return slab(q - 1 - k % q, 1 - k // q)

    def rs_copy(g, k):
        return remote(
            ssend.at[k, rows_of(g), :], srecv.at[k, rows_of(g), :], rs_s.at[g, k], rs_r.at[g, k], sibling
        )

    def ry_copy(g, j):
        return remote(
            srecv.at[q - 1 - j, rows_of(g), :], yrecv.at[j, rows_of(g), :],
            ry_s.at[g, j], ry_r.at[g, j], partner,
        )

    def rz_copy(g, j):
        goal, step = line(j), side(j)
        adjacent = (q + 1 - step * (goal - z)) // q
        spot = goal + (1 - step) // 2 * adjacent * (q - goal)
        return remote(
            yrecv.at[j, rows_of(g), :], zrecv.at[spot, rows_of(g), :],
            rz_s.at[g, j], rz_r.at[g, spot], {"tp": me + 2 * step},
        )

    def landed(g, spot):
        part = zrecv.at[spot, rows_of(g), :]
        remote(part, part, rz_s.at[g, 0], rz_r.at[g, spot], sibling).wait_recv()
        return zrecv[spot, rows_of(g), :].astype(F32)

    def combine(g, k):
        j = q - 1 - k % q
        rs_copy(g, k).wait_recv()
        mine = own[k % 2, 0:sizes[g], :]

        @pl.when(k < q)
        def _():
            srecv[k, rows_of(g), :] = (mine + srecv[k, rows_of(g), :].astype(F32)).astype(BF16)
            ry_copy(g, j).start()

        @pl.when(k >= q)
        def _():
            comb[j, rows_of(g), :] = mine + srecv[k, rows_of(g), :].astype(F32)

    def down(g, k):
        cols = chunk_rows(shard_of(k))
        rg = sizes[g]
        result = None
        for e in range(experts):
            part = jnp.dot(hq[e, 0:2 * rg, :], dbuf[e, :, cols], preferred_element_type=F32)
            part = part * coef[e, 0:2 * rg, 0:1] * ds_ref[:, cols][e:e + 1]
            result = part if result is None else result + part
        ssend[k, rows_of(g), :] = result[rg:].astype(BF16)
        rs_copy(g, k).start()
        own[k % 2, 0:rg, :] = result[0:rg]

        @pl.when(k > 0)
        def _():
            combine(g, k - 1)

    def finish(g, j):
        ry_copy(g, j).wait_recv()
        rows = rows_of(g)
        comb[j, rows, :] += yrecv[j, rows, :].astype(F32)

        @pl.when(j > 0)
        def _():
            behind = z - side(j)

            @pl.when((behind >= 0) & (behind < q))
            def _():
                comb[j, rows, :] += landed(g, line(j))

            yrecv[j, rows, :] = comb[j, rows, :].astype(BF16)
            rz_copy(g, j).start()

    def final(g):
        rows = rows_of(g)

        @pl.when(z > 0)
        def _():
            comb[0, rows, :] += landed(g, z)

        @pl.when(z < q - 1)
        def _():
            comb[0, rows, :] += landed(g, q)

        out_ref[rows, :] = comb[0, rows, :].astype(BF16)

    per_step = -(-n // (q - 1))
    last = groups - 1
    for g in range(groups):

        @pl.loop(0, q)
        def _(t):
            @pl.when(t > 0)
            def _():
                if g < last:
                    across(g + 1, t)

            @pl.when(t == 0)
            def _():
                compute(g, 0, True)

            @pl.when(t > 0)
            def _():
                compute(g, 2 * t, False)

            if g + 2 <= last:

                @pl.when(t == 1)
                def _():
                    begin(g + 2)

            if g == 0:

                @pl.when(t + 1 < q)
                def _():
                    across(0, t + 1)

                beside(0, t)
            else:

                @pl.when(t == q - 1)
                def _():
                    beside(g, t)

            if g < last:

                @pl.when(t > 0)
                def _():
                    beside(g + 1, t - 1)

            compute(g, 2 * t + 1, False)

            if g > 0:

                @pl.when(t == 1)
                def _():
                    requantize(g - 1)

                @pl.when(t >= 1)
                def _():
                    @pl.loop(0, per_step)
                    def _(i):
                        k = (t - 1) * per_step + i

                        @pl.when(k < n)
                        def _():
                            down(g - 1, k)

            if g > 1:
                finish(g - 2, q - 1 - t)

        if g == 0:
            for e in range(experts):
                down_copy(e).wait()
        hidden(g)
        if g > 0:
            combine(g - 1, n - 1)

    requantize(last)

    @pl.loop(0, n)
    def _(k):
        down(last, k)
        if last > 0:

            @pl.when(k >= q)
            def _():
                finish(last - 1, n - 1 - k)

    combine(last, n - 1)

    @pl.loop(0, q)
    def _(i):
        finish(last, q - 1 - i)

    for g in range(groups):
        final(g)

    meta_copy.wait_send()

    @pl.loop(1, n)
    def _(d):
        pk_copy(d).wait_send()

    for g in range(groups):
        guard_own(lambda up: own_copy(g, up).wait_send())

        @pl.loop(1, n)
        def _(d):
            hx_copy(g, d).wait_send()

        @pl.loop(0, n)
        def _(k):
            sib_copy(g, k).wait_send()
            rs_copy(g, k).wait_send()

        @pl.loop(0, q)
        def _(j):
            y_copy(g, slab(j, 0)).wait_send()
            ry_copy(g, j).wait_send()

        @pl.loop(1, q)
        def _(j):
            guard_slabs(
                j, lambda p, step: guard_relay(g, p, step, lambda copy: copy.wait_send())
            )
            rz_copy(g, j).wait_send()


def per_device(
    n,
    tokens, smooth_in, expert_ids, gate_fixed, slots,
    w_gate, w_up, w_down, gate_scale, up_scale, smooth_mid, down_scale,
):
    q = n // 2
    experts, features, width = w_gate.shape
    block, depth = tokens.shape
    sizes = tuple(block * part // sum(SPLIT) for part in SPLIT)
    groups = len(sizes)
    rows_m = 2 * max(sizes)
    packed = width % LANES == 0
    halves = 1 if packed else 2
    cols = 2 * width if packed else width
    vmem = pl.BlockSpec(memory_space=pltpu.VMEM)
    hbm = pl.BlockSpec(memory_space=pl.ANY)
    dma = pltpu.SemaphoreType.DMA
    slab = (block, depth)
    return pl.pallas_call(
        functools.partial(kernel, n, 3 * block // 4, sizes),
        out_shape=jax.ShapeDtypeStruct((block, depth), BF16),
        in_specs=[vmem] * 5 + [hbm] * 3 + [vmem] * 4,
        out_specs=vmem,
        scratch_shapes=[
            pltpu.VMEM((n, 2, *slab), BF16),
            pltpu.VMEM((rows_m, depth), BF16),
            pltpu.VMEM((halves, experts, features, cols), BF16),
            pltpu.VMEM((experts, width, features), BF16),
            pltpu.VMEM((halves, experts, rows_m, cols), F32),
            pltpu.VMEM((experts, rows_m, width), F32),
            pltpu.VMEM((experts, rows_m, width), BF16),
            pltpu.VMEM((4, 8, block), F32),
            pltpu.VMEM((2, block, LANES), F32),
            pltpu.VMEM((experts, rows_m, LANES), F32),
            pltpu.VMEM((n + 8, 1, block + depth), F32),
            pltpu.VMEM((groups, n + 8, experts, rows_m), F32),
            pltpu.VMEM((rows_m, LANES), F32),
            pltpu.VMEM((2, max(sizes), depth), F32),
            pltpu.VMEM((n, *slab), BF16),
            pltpu.VMEM((n, *slab), BF16),
            pltpu.VMEM((q, *slab), F32),
            pltpu.VMEM((q, *slab), BF16),
            pltpu.VMEM((q + 1, *slab), BF16),
            dma((n, 2)), dma((experts,)), dma((n,)), dma((n,)), dma((groups, n)), dma((groups, n)), dma, dma,
            dma((groups, 2)), dma((groups, q)), dma((groups, q)), dma((groups, n)), dma((groups, n)), dma((groups, n)),
            dma((groups, n)), dma((groups, n)), dma((groups, q)), dma((groups, q)), dma((groups, q)), dma((groups, q + 1)),
        ],
        compiler_params=pltpu.CompilerParams(
            collective_id=0, has_side_effects=True, vmem_limit_bytes=67043328
        ),
    )(
        tokens, smooth_in[None, :], expert_ids.T, gate_fixed.T, slots.T,
        w_gate, w_up, w_down, gate_scale, up_scale, smooth_mid, down_scale,
    )


def solution(mesh):
    n = mesh.shape["tp"]
    in_specs = (
        P(("rep", "exp"), "tp"),
        P("tp"),
        P(("rep", "exp"), None),
        P(("rep", "exp"), None),
        P(("rep", "exp"), None),
        P("exp", None, "tp"),
        P("exp", None, "tp"),
        P("exp", "tp", None),
        P("exp", "tp"),
        P("exp", "tp"),
        P("exp", "tp"),
        P("exp", None),
    )
    out_specs = P(("rep", "exp"), "tp")
    return jax.shard_map(
        functools.partial(per_device, n), mesh=mesh, in_specs=in_specs, out_specs=out_specs, check_vma=False
    )
```
